256 devices in a mesh: dp: 64 (over z, y, core), tp: 4 (over x).
Axes of the slice: x: 4, y: 4, z: 8, core: 2. Of those that a mesh axis runs over, the one named last changes fastest.
Arguments:
- partial_up: bfloat16 [64, 1024, 4096], P('dp', None, 'tp'), may hold values from -8 to 8
- partial_down: bfloat16 [64, 4096, 1024], P('dp', 'tp'), may hold values from -8 to 8
- partial_norm: bfloat16 [64, 1024], P('dp'), may hold values from -16 to 16
- master_up: float32 [1024, 4096], P('dp', 'tp'), may hold values from -0.5 to 0.5
- master_down: float32 [4096, 1024], P('tp', 'dp'), may hold values from -0.25 to 0.25
- master_norm: float32 [1024], P('dp'), may hold values from 0.25 to 1.75
- memory_up: float32 [1024, 4096], P('dp', 'tp'), may hold values from 0.0001953125 to 0.001953125
- memory_down: float32 [4096, 1024], P('tp', 'dp'), may hold values from 4.8828126e-05 to 0.00048828125
- memory_norm: float32 [1024], P('dp'), may hold values from 0.05 to 0.8
Outputs:
- compute_up: bfloat16 [1024, 4096], P(None, 'tp')
- compute_down: bfloat16 [4096, 1024], P('tp')
- compute_norm: bfloat16 [1024], replicated
- stepped_up: float32 [1024, 4096], P('dp', 'tp')
- stepped_down: float32 [4096, 1024], P('tp', 'dp')
- stepped_norm: float32 [1024], P('dp')
- state_new_up: float32 [1024, 4096], P('dp', 'tp')
- state_new_down: float32 [4096, 1024], P('tp', 'dp')
- state_new_norm: float32 [1024], P('dp')
The draws below stay inside these ranges and needn't reach their ends.
All inputs are finite; a program needn't handle non-finite values.
Results may differ from the reference program's by a relative error of at most 0.001.
Values may be sent and summed in bfloat16 or wider, within the bound.
No kernel may reach another device: no remote copies, remote signals or barrier semaphores. Data moves between devices by JAX's collectives and lax.ppermute only.
A program may use at most 64 MiB of HBM per device.

```python
import jax
import jax.numpy as jnp
from jax import lax

WIDTH = 1024
INNER = 4096
REPLICAS = 64


def raised(values, own_key, source, target, shards_of, factor):
    def block_of(axis_at):
        return (jnp.arange(values.shape[axis_at]) // (values.shape[axis_at] // shards_of)).reshape((-1,) + (1,) * (values.ndim - 1 - axis_at))

    near = jax.random.permutation(own_key, shards_of)[block_of(target)]
    far = (block_of(target) + shards_of // 2) % shards_of
    return jnp.where((block_of(source) == near) | (block_of(source) == far), factor * values, values)


def block_levels(rng, extent, cuts, low, largest):
    def one(dim, shards_of):
        steps = jax.random.uniform(jax.random.fold_in(jax.random.fold_in(rng, 6), dim), (shards_of,), jnp.float32, low / len(cuts), largest / len(cuts))
        return jnp.repeat(jnp.exp(steps), extent[dim] // shards_of).reshape((-1,) + (1,) * (len(extent) - dim - 1))

    factor_of = one(*cuts[0])
    for cut in cuts[1:]:
        factor_of = factor_of * one(*cut)
    return factor_of


def noise_with(key, extent, width, limit, shards, heavy, kind=jnp.bfloat16):
    array = width * jax.random.normal(key, extent, jnp.float32)
    if shards:
        array = array * block_levels(key, extent, shards, -0.22, 0.18)
    return jnp.clip(raised(array, jax.random.fold_in(key, 3), *heavy), -limit, limit).astype(kind)


def setup_inputs(seed: int = 0) -> dict:
    streams_of = jax.random.split(jax.random.key(seed), 10)
    partial_up = noise_with(streams_of[0], (REPLICAS, WIDTH, INNER), 0.5, 8.0, ((0, 64), (2, 4)), (0, 1, 64, 4.0))
    partial_down = noise_with(streams_of[1], (REPLICAS, INNER, WIDTH), 0.5, 8.0, ((0, 64), (1, 4)), (0, 2, 64, 4.0))
    partial_norm = noise_with(streams_of[2], (REPLICAS, WIDTH), 1.0, 16.0, ((0, 64),), (0, 1, 64, 4.0))
    master_up = noise_with(streams_of[3], (WIDTH, INNER), WIDTH ** -0.5, 0.5, ((0, 64), (1, 4)), (1, 0, 64, 4.0), jnp.float32)
    master_down = noise_with(streams_of[4], (INNER, WIDTH), INNER ** -0.5, 0.25, ((0, 4), (1, 64)), (0, 1, 64, 4.0), jnp.float32)
    master_norm = jnp.clip(1.0 + 0.15 * jax.random.normal(streams_of[5], (WIDTH,), jnp.float32), 0.25, 1.75)
    memory_up = jnp.clip(0.0001953125 + 0.0017578125 * jax.random.uniform(streams_of[6], (WIDTH, INNER), jnp.float32) ** block_levels(streams_of[6], (WIDTH, INNER), ((0, 64), (1, 4)), -0.2, 0.2), 0.0001953125, 0.001953125)
    memory_down = jnp.clip(4.882812572759576e-05 + 0.0004394531 * jax.random.uniform(streams_of[7], (INNER, WIDTH), jnp.float32) ** block_levels(streams_of[7], (INNER, WIDTH), ((0, 4), (1, 64)), -0.2, 0.2), 4.882812572759576e-05, 0.00048828125)
    memory_norm = jnp.clip(0.05 + 0.75 * jax.random.uniform(streams_of[8], (WIDTH,), jnp.float32) ** block_levels(streams_of[8], (WIDTH,), ((0, 64),), -0.2, 0.2), 0.05, 0.8)
    return {"partial_up": partial_up, "partial_down": partial_down, "partial_norm": partial_norm, "master_up": master_up, "master_down": master_down, "master_norm": master_norm, "memory_up": memory_up, "memory_down": memory_down, "memory_norm": memory_norm}


learn_rate = 0.025
hold_rate = 0.8

def reference(partial_up, partial_down, partial_norm, master_up, master_down, master_norm, memory_up, memory_down, memory_norm):
    mean_up = lax.optimization_barrier(jnp.sum(partial_up.astype(jnp.float32), axis=0)) * REPLICAS ** (-0.5)
    mean_down = lax.optimization_barrier(jnp.sum(partial_down.astype(jnp.float32), axis=0)) * REPLICAS ** (-0.5)
    mean_norm = lax.optimization_barrier(jnp.sum(partial_norm.astype(jnp.float32), axis=0)) * REPLICAS ** (-0.5)
    ratio_up = jnp.sqrt(lax.optimization_barrier(jnp.sum(master_up * master_up, axis=1, keepdims=True))) * lax.rsqrt(lax.optimization_barrier(jnp.sum(mean_up * mean_up, axis=1, keepdims=True)) + 1e-06)
    mean_up = mean_up * ratio_up
    ratio_down = jnp.sqrt(lax.optimization_barrier(jnp.sum(master_down * master_down, axis=0, keepdims=True))) * lax.rsqrt(lax.optimization_barrier(jnp.sum(mean_down * mean_down, axis=0, keepdims=True)) + 1e-06)
    mean_down = mean_down * ratio_down
    state_new_up = hold_rate * memory_up + (1.0 - hold_rate) * mean_up * mean_up
    stepped_up = master_up - learn_rate * mean_up * lax.rsqrt(state_new_up + 1e-06)
    state_new_down = hold_rate * memory_down + (1.0 - hold_rate) * mean_down * mean_down
    stepped_down = master_down - learn_rate * mean_down * lax.rsqrt(state_new_down + 1e-06)
    state_new_norm = hold_rate * memory_norm + (1.0 - hold_rate) * mean_norm * mean_norm
    stepped_norm = master_norm - learn_rate * mean_norm * lax.rsqrt(state_new_norm + 1e-06)
    compute_up = stepped_up.astype(jnp.bfloat16)
    compute_down = stepped_down.astype(jnp.bfloat16)
    compute_norm = stepped_norm.astype(jnp.bfloat16)
    return (compute_up, compute_down, compute_norm, stepped_up, stepped_down, stepped_norm, state_new_up, state_new_down, state_new_norm)
```

```python
import jax
import jax.numpy as jnp
from jax import lax
from jax.experimental.layout import Layout, with_layout_constraint
from jax.sharding import Mesh
from jax.sharding import PartitionSpec as P

from jax.experimental import pallas as pl
from jax.experimental.pallas import tpu as pltpu


DP = ("z", "y", "c")
Z, Y, C = 8, 4, 2
LANES = 128

learn_rate = 0.025
hold_rate = 0.8


def index_of(z, y, c):
    return (z % Z * Y + y % Y) * C + c


def hop(value, axis, by=1):
    pairs = []
    for z in range(Z):
        for y in range(Y):
            for c, way in ((0, by), (1, -by)):
                to = (z + way, y) if axis == "z" else (z, y + way)
                pairs.append((index_of(z, y, c), index_of(*to, c)))
    return lax.ppermute(value, DP, pairs)


def swapped(value, axis, bit=1):
    size = lax.axis_size(axis)
    return lax.ppermute(value, axis, [(i, i ^ bit) for i in range(size)])


def shift(value, axis, by):
    size = lax.axis_size(axis)
    return lax.ppermute(value, axis, [(i, (i + by) % size) for i in range(size)])


def at(array, *places):
    starts, sizes, kept = [], [], []
    for dim, size in enumerate(array.shape):
        place = places[dim] if dim < len(places) else None
        starts.append(0 if place is None else place)
        sizes.append(size if place is None else 1)
        if place is None:
            kept.append(size)
    return lax.dynamic_slice(array, starts, sizes).reshape(kept)


def stepped_of(mean, master, memory):
    state_new = hold_rate * memory + (1.0 - hold_rate) * mean * mean
    return master - learn_rate * mean * lax.rsqrt(state_new + 1e-06), state_new


def ratio_of(mean, master):
    sizes = jnp.stack([jnp.sum(master * master, axis=1), jnp.sum(mean * mean, axis=1)])
    sizes = sizes + shift(sizes, "x", 1) + shift(sizes, "x", 3) + shift(sizes, "x", 2)
    return (jnp.sqrt(sizes[0]) * lax.rsqrt(sizes[1] + 1e-06))[:, None]


def summed(mine, other, axes, lanes=None):
    z, y, core = (lax.axis_index(a) for a in DP)
    way, peer = 1 - 2 * core, 1 - core
    sizes, spots = {"z": Z, "y": Y}, {"z": z, "y": y}
    first, second = axes
    far, near = sizes[first] // 2, sizes[second] // 2

    def on(axis, k):
        return lax.rem(spots[axis] + way * k + sizes[axis], sizes[axis])

    def own(*spot):
        piece = at(mine, *spot).astype(jnp.float32) + at(other, *spot).astype(jnp.float32)
        if lanes is not None:
            piece = jnp.concatenate([piece, at(lanes, *spot)], axis=-1)
        return lax.optimization_barrier(piece)

    def rows(k, parity):
        spot = on(first, k)
        return own(spot, None, parity) if first == "z" else own(None, spot, parity)

    same, rest = yield rows(far, core), rows(far - 1, peer)
    for left in range(far, 0, -1):
        same = hop(same, first)
        if left > 1:
            rest = hop(rest, first)
            same = same + rows(left - 1, core)
            if left > 2:
                rest = rest + rows(left - 2, peer)
            else:
                over_rest = swapped(rest, "c")
    over_same = swapped(same, "c")

    def total(k, is_same):
        spot = on(second, k)
        here, there, parity = (same, over_rest, core) if is_same else (rest, over_same, peer)
        both = (spots[first], spot) if first == "z" else (spot, spots[first])
        return at(here, spot) + at(there, spot) + own(*both, parity)

    kept, traded = hop(total(near, True), second, near), None
    for k in range(1, near):
        pair = jnp.stack([total(k, True), total(k, False)])
        pair = hop(pair, second, k)
        kept = kept + pair[0]
        traded = pair[1] if traded is None else traded + pair[1]
    yield total(0, True) + kept + swapped(traded, "c")


def by_parity(mine, other):
    first = lax.axis_index("c") == 0
    return jnp.stack([jnp.where(first, mine, other), jnp.where(first, other, mine)])


def chip_lines(block):
    y, core = lax.axis_index("y"), lax.axis_index("c")
    chip = by_parity(block, swapped(block, "c"))
    near = hop(chip, "y")
    far = hop(at(chip, core), "y", 2)
    other_near, other_far = swapped(near, "c"), swapped(far, "c")
    way = 1 - 2 * core
    offset = lax.rem(way * (lax.iota(jnp.int32, Y) - y) + 2 * Y, Y).reshape(Y, 1, 1, 1)
    far = by_parity(far, other_far)
    return jnp.where(
        offset == 0, chip, jnp.where(offset == 3, near, jnp.where(offset == 1, other_near, far))
    )


def over_z(lines):
    z, core = lax.axis_index("z"), lax.axis_index("c")
    way = 1 - 2 * core
    wide = lines.shape[-1]
    pieces, places = [lines], [z]
    travelling = lines
    for k in range(1, Z // 2):
        travelling = hop(travelling, "z")
        traded = swapped(travelling, "c")
        pieces += [travelling, traded]
        places += [lax.rem(z - way * k + Z, Z), lax.rem(z + way * k + Z, Z)]
    half = at(travelling.transpose(1, 0, 2, 3), core)
    half = hop(half, "z")
    pieces += [half, swapped(half, "c")]
    places += [lax.rem(z + Z // 2, Z), core]
    return jnp.stack(places).astype(jnp.int32), [p.reshape(-1, wide) for p in pieces]


def stage_all(places, pieces, stage, sems):
    deep = stage.shape[0] // Z
    rows = deep // (Y * C)
    copies = []
    for i, piece in enumerate(pieces):
        if piece.shape[0] == deep:
            to = pl.ds(pl.multiple_of(places[i] * deep, deep), deep)
            copies.append((piece, stage.at[to, :]))
        else:
            parity = places[len(pieces) - 1]
            if i == len(pieces) - 1:
                parity = 1 - parity
            for y in range(Y):
                at_row = places[len(pieces) - 2] * deep + (y * C + parity) * rows
                to = pl.ds(pl.multiple_of(at_row, rows), rows)
                copies.append((piece.at[pl.ds(y * rows, rows), :], stage.at[to, :]))
    started = [pltpu.make_async_copy(a, b, sems.at[i]) for i, (a, b) in enumerate(copies)]
    for copy in started:
        copy.start()
    for copy in started:
        copy.wait()


def up_kernel(places, *refs):
    *pieces, out, beside, stage, sems, out_sems = refs
    stage_all(places, pieces, stage, sems)
    wide = out.shape[1]
    copies = [
        pltpu.make_async_copy(stage.at[:, pl.ds(0, wide)], out, out_sems.at[0]),
        pltpu.make_async_copy(stage.at[:, pl.ds(wide, LANES)], beside, out_sems.at[1]),
    ]
    for copy in copies:
        copy.start()
    for copy in copies:
        copy.wait()


def down_kernel(places, *refs):
    *pieces, out, stage, turned, sems, out_sems = refs
    stage_all(places, pieces, stage, sems)
    deep = stage.shape[0] // Z
    for z in range(Z):
        columns = pl.ds(z * deep, deep)
        turned[:, columns] = stage[columns, :].T
    copy = pltpu.make_async_copy(turned, out, out_sems.at[0])
    copy.start()
    copy.wait()


def placed(kernel, places, pieces, outs, scratch):
    deep, wide = pieces[0].shape
    n_copies = len(pieces) - 2 + 2 * Y
    out_bytes = sum(o.size * o.dtype.itemsize for o in outs)
    return pl.pallas_call(
        kernel,
        out_shape=outs,
        in_specs=[pl.BlockSpec(memory_space=pltpu.SMEM)]
        + [pl.BlockSpec(memory_space=pl.ANY)] * len(pieces),
        out_specs=[pl.BlockSpec(memory_space=pl.ANY)] * len(outs),
        scratch_shapes=[
            pltpu.VMEM((Z * deep, wide), pieces[0].dtype),
            *scratch,
            pltpu.SemaphoreType.DMA((n_copies,)),
            pltpu.SemaphoreType.DMA((len(outs),)),
        ],
        cost_estimate=pl.CostEstimate(
            flops=out_bytes, bytes_accessed=2 * out_bytes, transcendentals=0
        ),
        compiler_params=pltpu.CompilerParams(vmem_limit_bytes=16 * 2**20),
    )(places, *pieces)


def local(
    partial_up,
    partial_down,
    partial_norm,
    master_up,
    master_down,
    master_norm,
    memory_up,
    memory_down,
    memory_norm,
):
    mean_rate = lax.axis_size(DP) ** (-0.5)
    rows = master_norm.shape[0]
    width = partial_up.shape[2]

    cut = (Z, Y, C, rows, width)
    mine_up = partial_up[0]
    other_up = swapped(mine_up, "c")
    other_norm = swapped(partial_norm, "c")
    vector = partial_norm.astype(jnp.float32) + other_norm.astype(jnp.float32)
    lanes = jnp.broadcast_to(vector.reshape(*cut[:4], 1), (*cut[:4], LANES))
    lanes = lax.optimization_barrier(lanes)
    mine_down = with_layout_constraint(partial_down[0].T, Layout((0, 1)))
    other_down = swapped(mine_down, "c")
    up_of = summed(mine_up.reshape(cut), other_up.reshape(cut), "yz", lanes)
    first_up = next(up_of)
    mine_down, other_down, first_up = lax.optimization_barrier((mine_down, other_down, first_up))
    down_of = summed(mine_down.reshape(cut), other_down.reshape(cut), "zy")
    down = down_of.send(next(down_of))
    up = up_of.send(first_up)

    master_down, memory_down = master_down.T, memory_down.T
    mean_up = up[:, :width] * mean_rate
    mean_norm = up[:, width:] * mean_rate
    mean_down = down * mean_rate
    ratio = ratio_of(
        jnp.concatenate([mean_up, mean_down]), jnp.concatenate([master_up, master_down])
    )
    mean_up = mean_up * ratio[:rows]
    stepped_up, state_new_up = stepped_of(mean_up, master_up, memory_up)
    mean_down = mean_down * ratio[rows:]
    stepped_down, state_new_down = stepped_of(mean_down, master_down, memory_down)

    across = jnp.broadcast_to(master_norm[:, None], mean_norm.shape)
    stepped_norm, state_new_norm = stepped_of(
        mean_norm, across, jnp.broadcast_to(memory_norm[:, None], mean_norm.shape)
    )

    lines = jnp.concatenate([stepped_down, stepped_up, stepped_norm], axis=1)
    lines = chip_lines(lines.astype(jnp.bfloat16))
    places, pieces = over_z(lines[..., :width])
    whole = jax.ShapeDtypeStruct((width, Z * pieces[0].shape[0]), jnp.bfloat16)
    (compute_down,) = placed(
        down_kernel, places, pieces, [whole], [pltpu.VMEM(whole.shape, whole.dtype)]
    )
    places, pieces = over_z(lines[..., width:])
    deep = Z * pieces[0].shape[0]
    compute_up, norm_lanes = placed(
        up_kernel,
        places,
        pieces,
        [jax.ShapeDtypeStruct((deep, n), jnp.bfloat16) for n in (width, LANES)],
        [],
    )
    norm_lanes = norm_lanes.reshape(-1, LANES, LANES)
    diagonal = lax.broadcasted_iota(jnp.int32, (1, LANES, LANES), 1) == lax.broadcasted_iota(
        jnp.int32, (1, LANES, LANES), 2
    )
    compute_norm = jnp.sum(jnp.where(diagonal, norm_lanes.astype(jnp.float32), 0.0), axis=1)
    compute_norm = compute_norm.astype(jnp.bfloat16).reshape(-1)
    stepped_norm, state_new_norm = stepped_norm[:, 0], state_new_norm[:, 0]
    return (
        compute_up,
        compute_down,
        compute_norm,
        stepped_up,
        stepped_down.T,
        stepped_norm,
        state_new_up,
        state_new_down.T,
        state_new_norm,
    )


def solution(mesh):
    finer = Mesh(mesh.devices.reshape(Z, Y, C, mesh.shape["tp"]), (*DP, "x"))
    return jax.shard_map(
        local,
        mesh=finer,
        in_specs=(
            P(DP, None, "x"),
            P(DP, "x", None),
            P(DP, None),
            P(DP, "x"),
            P("x", DP),
            P(DP),
            P(DP, "x"),
            P("x", DP),
            P(DP),
        ),
        out_specs=(
            P(None, "x"),
            P("x", None),
            P(),
            P(DP, "x"),
            P("x", DP),
            P(DP),
            P(DP, "x"),
            P("x", DP),
            P(DP),
        ),
        check_vma=False,
    )
```
